32 devices in a mesh: grp: 2 (over x), dom: 16 (over z, y, core).
Axes of the slice: x: 2, y: 2, z: 4, core: 2. Of those that a mesh axis runs over, the one named last changes fastest.
Arguments:
- surplus: float32 [48, 64, 4096], P('grp', None, 'dom'), may hold values from -40 to 40
- levels: int32 [48, 3], P('grp'), may hold values from 0 to 3
Outputs:
- updated: float32 [48, 64, 4096], P('grp', None, 'dom')
- coefficients: float32 [48], replicated
The draws below stay inside these ranges and needn't reach their ends.
All inputs are finite; a program needn't handle non-finite values.
Results may differ from the reference program's by a relative error of at most 0.0003.
Values sent between devices are 32-bit elements; how exact they have to be, the bound alone decides.
A program may use at most 64 MiB of HBM per device.

```python
import math
import jax
import jax.numpy as jnp
from jax import lax

GRIDS = 48
SUBSP = 64
NC = 4096


def draw_surplus(key, part):
    keys = jax.random.split(jax.random.fold_in(key, 11), 4)
    index = jnp.arange(SUBSP, dtype=jnp.int32)
    level_sum = (index // 16 + index // 4 % 4 + index % 4).astype(jnp.float32)
    position = jnp.arange(NC, dtype=jnp.float32) / float(max(NC - 1, 1))
    common = jax.random.normal(keys[0], (SUBSP, NC), jnp.float32)
    single = jax.random.normal(keys[1], (GRIDS, SUBSP, NC), jnp.float32)
    gains = jnp.exp(jax.random.uniform(keys[2], (GRIDS, SUBSP, 1), jnp.float32, math.log(0.5), math.log(2.0)))
    spread = jnp.exp(jax.random.uniform(keys[3], (GRIDS, SUBSP, 1), jnp.float32, math.log(0.4), math.log(1.2)))
    envelope = 3.0 ** position / math.sqrt(3.0)
    amplitude = 1.5 * 10.0 ** (-level_sum / 9.0)
    values = envelope[None, None, :] * amplitude[None, :, None] * (gains * common[None] + spread * single)
    return jnp.clip(values, -40.0, 40.0).astype(jnp.float32)


def set_ends(result, own_key, smallest, high):
    dims = result.shape
    index_at = [jax.random.randint(jax.random.fold_in(own_key, axis), (), 0, dims[axis]) for axis in range(len(dims))]
    result = result.at[tuple(index_at)].set(smallest)
    longest = dims.index(max(dims))
    index_at[longest] = (index_at[longest] + 1) % dims[longest]
    return result.at[tuple(index_at)].set(high)


def setup_inputs(seed: int = 0) -> dict:
    arg_keys = jax.random.split(jax.random.key(seed), 3)
    return {
        "surplus": draw_surplus(jax.random.fold_in(arg_keys[2], 71), 0),
        "levels": set_ends(jax.random.randint(arg_keys[1], (GRIDS, 3), 0, 4), jax.random.fold_in(arg_keys[1], 1), 0, 3).astype(jnp.int32),
    }


def owned(levels, count):
    indices = jnp.arange(count, dtype=jnp.int32)
    digits = jnp.stack([indices // 16, indices // 4 % 4, indices % 4])
    return jnp.all(digits[None] <= levels[:, :, None], axis=1).astype(jnp.float32)

def solve_weights(gram_matrix):
    number = gram_matrix.shape[0]
    diagonal_part = jnp.diagonal(gram_matrix) + 1e-06
    scaling = 1.0 / jnp.sqrt(diagonal_part)
    system = scaling[:, None] * gram_matrix * scaling[None, :] + 0.1 * jnp.eye(number, dtype=jnp.float32)
    factor = jnp.linalg.cholesky(system)
    target = jnp.sqrt(diagonal_part)[:, None]
    halfway = lax.linalg.triangular_solve(factor, target, left_side=True, lower=True)
    weights = lax.linalg.triangular_solve(factor, halfway, left_side=True, lower=True, transpose_a=True)
    return scaling * weights[:, 0]

def reference(surplus, levels):
    owners = owned(levels, SUBSP)
    masked = surplus * owners[:, :, None]
    flattened = masked.reshape(GRIDS, -1)
    gram_matrix = jnp.dot(flattened.astype(jnp.float32), flattened.T.astype(jnp.float32), precision=lax.Precision.HIGHEST, preferred_element_type=jnp.float32)
    coefficients = solve_weights(gram_matrix)
    combined = jnp.tensordot(coefficients, masked, axes=1, precision=lax.Precision.HIGHEST)
    updated = owners[:, :, None] * combined[None]
    return (updated, coefficients)
```

```python
import functools

import jax
import jax.numpy as jnp
from jax import lax
from jax.experimental import pallas as pl
from jax.experimental.pallas import tpu as pltpu
from jax.sharding import PartitionSpec as P

MESH = pl.DeviceIdType.MESH
ROWS = 8
F32 = jnp.float32


def radices_of(size):
    out = []
    while size > 1:
        for r in (4, 2, 3, 5, 7, size):
            if size % r == 0:
                out.append(r)
                size //= r
                break
    return out


def split3(x):
    hi = x.astype(jnp.bfloat16)
    rest = x - hi.astype(F32)
    mid = rest.astype(jnp.bfloat16)
    lo = (rest - mid.astype(F32)).astype(jnp.bfloat16)
    return jnp.concatenate([hi, mid, lo], axis=0)


def kernel(groups, radices, local, subs, surplus, levels, comb_out, coef_out, *scratch):
    stages = len(radices)
    (xb, lev, lbc, prod, cbuf, local_sem, lev_send, lev_recv, x_send, x_recv, c_send, c_recv) = scratch[:12]
    slots = scratch[12:12 + stages]
    s_send = scratch[12 + stages:12 + 2 * stages]
    s_recv = scratch[12 + 2 * stages:12 + 3 * stages]
    grids = groups * local
    half = xb.shape[-1]
    chunks = subs // ROWS
    g = lax.axis_index("grp")
    d = lax.axis_index("dom")

    members = []
    stride = 1
    for t, r in enumerate(radices):
        digit = lax.rem(d // stride, r)
        base = d - digit * stride
        if t == 0:
            n = groups * r
            mine = g * r + digit
            device = functools.partial(lambda b, r_, q: (q // r_, b + lax.rem(q, r_)), base, r)
        else:
            n = r
            mine = digit
            device = functools.partial(lambda b, st, q: (g, b + q * st), base, stride)
        members.append((n, mine, device))
        stride *= r

    barrier = pltpu.get_barrier_semaphore()
    count = 0
    for n, mine, device in members:
        for k in range(1, n):
            q = lax.rem(mine + k, n)
            pl.semaphore_signal(barrier, inc=1, device_id=device(q), device_id_type=MESH)
            count += 1

    own_cells = pl.ds(pl.multiple_of(g * half, half), half)
    own_copy = pltpu.make_async_copy(
        surplus.at[:, :, own_cells], xb.at[pl.ds(g * local, local)], local_sem
    )
    own_copy.start()
    pl.semaphore_wait(barrier, count)

    def lev_copy(k):
        q = lax.rem(g + k, groups)
        return pltpu.make_async_remote_copy(
            src_ref=levels, dst_ref=lev.at[g], send_sem=lev_send.at[k], recv_sem=lev_recv.at[g],
            device_id=(q, d), device_id_type=MESH,
        )

    def x_copy(k, ch):
        q = lax.rem(g + k, groups)
        rows = pl.ds(pl.multiple_of(ch * ROWS, ROWS), ROWS)
        return pltpu.make_async_remote_copy(
            src_ref=surplus.at[:, rows, pl.ds(pl.multiple_of(q * half, half), half)],
            dst_ref=xb.at[pl.ds(g * local, local), rows],
            send_sem=x_send.at[k, ch], recv_sem=x_recv.at[g, ch],
            device_id=(q, d), device_id_type=MESH,
        )

    def x_arrival(k, ch):
        q = lax.rem(g + k, groups)
        rows = pl.ds(pl.multiple_of(ch * ROWS, ROWS), ROWS)
        block = xb.at[pl.ds(q * local, local), rows]
        return pltpu.make_async_remote_copy(
            src_ref=block, dst_ref=block, send_sem=x_send.at[k, ch], recv_sem=x_recv.at[q, ch],
            device_id=(q, d), device_id_type=MESH,
        )

    for k in range(1, groups):
        lev_copy(k).start()
    for ch in range(chunks):
        for k in range(1, groups):
            x_copy(k, ch).start()

    lev[g] = levels[...]
    for k in range(1, groups):
        q = lax.rem(g + k, groups)
        pltpu.make_async_remote_copy(
            src_ref=lev.at[q], dst_ref=lev.at[q], send_sem=lev_send.at[k], recv_sem=lev_recv.at[q],
            device_id=(q, d), device_id_type=MESH,
        ).wait_recv()
    for h in range(groups):
        for axis in range(3):
            lbc[axis, pl.ds(h * local, local), :] = jnp.broadcast_to(
                lev[h, :, axis:axis + 1], (local, 128)
            )
    prod[...] = jnp.zeros_like(prod)
    own_copy.wait()
    flat = xb.reshape(grids * subs, half)

    def gram_chunk(ch, carry):
        for k in range(1, groups):
            x_arrival(k, ch).wait_recv()
        lev0, lev1, lev2 = lbc[0], lbc[1], lbc[2]
        total = jnp.zeros(prod.shape, F32)
        for pair in range(0, ROWS, 2):
            parts = []
            for k in range(pair, pair + 2):
                s = ch * ROWS + k
                x = flat[pl.ds(s, grids, stride=subs), :]
                keep = (lev0 >= s // 16) & (lev1 >= lax.rem(s // 4, 4)) & (lev2 >= k % 4)
                keep = jnp.concatenate([keep] * (half // 128), axis=1) if half > 128 else keep
                parts.append(jnp.where(keep, x, 0.0))
            y = split3(jnp.concatenate(parts, axis=1))
            total += lax.dot_general(y, y, (((1,), (1,)), ((), ())), preferred_element_type=F32)
        prod[...] += total
        return carry

    lax.fori_loop(0, chunks, gram_chunk, 0)

    part = jnp.zeros((grids, grids), F32)
    for a in reversed(range(3)):
        for b in reversed(range(3)):
            part += prod[a * grids:(a + 1) * grids, b * grids:(b + 1) * grids]
    value = jnp.concatenate([part, jnp.zeros((grids, 128 - grids), F32)], axis=1)

    for t, (n, mine, device) in enumerate(members):
        buf, send, recv = slots[t], s_send[t], s_recv[t]
        buf[mine] = value
        copies = []
        for k in range(1, n):
            q = lax.rem(mine + k, n)
            copy = pltpu.make_async_remote_copy(
                src_ref=buf.at[mine], dst_ref=buf.at[mine], send_sem=send.at[k], recv_sem=recv.at[mine],
                device_id=device(q), device_id_type=MESH,
            )
            copy.start()
            copies.append(copy)
        for k in range(1, n):
            q = lax.rem(mine + k, n)
            pltpu.make_async_remote_copy(
                src_ref=buf.at[q], dst_ref=buf.at[q], send_sem=send.at[k], recv_sem=recv.at[q],
                device_id=device(q), device_id_type=MESH,
            ).wait_recv()
        value = buf[0]
        for q in range(1, n):
            value = value + buf[q]
        for copy in copies:
            copy.wait_send()

    row = lax.broadcasted_iota(jnp.int32, (grids, 128), 0)
    col = lax.broadcasted_iota(jnp.int32, (grids, 128), 1)
    eye = row == col
    diag = jnp.where(eye, value, 0.0)
    diag_col = jnp.sum(diag, axis=1, keepdims=True) + 1e-06
    diag_row = jnp.sum(diag, axis=0, keepdims=True) + 1e-06
    scale_col = 1.0 / jnp.sqrt(diag_col)
    scale_row = 1.0 / jnp.sqrt(diag_row)
    system = scale_col * value * scale_row + jnp.where(eye, 0.1, 0.0)
    system = jnp.where(col == grids, jnp.sqrt(diag_col), jnp.where(col < grids, system, 0.0))
    for k in range(grids):
        pivot_row = system[k:k + 1, :]
        inverse = 1.0 / pivot_row[:, k:k + 1]
        factor = jnp.where(row[:, 0:1] == k, 0.0, system[:, k:k + 1])
        system = system - factor * (pivot_row * inverse)
    final = jnp.sum(jnp.where(eye, system, 0.0), axis=1, keepdims=True)
    coef = scale_col * (system[:, grids:grids + 1] / final)
    coef_wide = jnp.broadcast_to(coef, (grids, 128))
    coef_out[...] = jnp.sum(jnp.where(eye, coef_wide, 0.0), axis=0, keepdims=True)[:, :grids]

    sub = lax.broadcasted_iota(jnp.int32, (subs, half), 0)
    dig0, dig1, dig2 = sub // 16, lax.rem(sub // 4, 4), lax.rem(sub, 4)
    acc = jnp.zeros((subs, half), F32)
    for i in range(grids):
        keep = (
            (lbc[0, i:i + 1, 0:1] >= dig0)
            & (lbc[1, i:i + 1, 0:1] >= dig1)
            & (lbc[2, i:i + 1, 0:1] >= dig2)
        )
        acc += jnp.where(keep, coef_wide[i:i + 1, 0:1], 0.0) * xb[i]
    cbuf[g] = acc
    for k in range(1, groups):
        q = lax.rem(g + k, groups)
        pltpu.make_async_remote_copy(
            src_ref=cbuf.at[g], dst_ref=cbuf.at[g], send_sem=c_send.at[k], recv_sem=c_recv.at[g],
            device_id=(q, d), device_id_type=MESH,
        ).start()
    for k in range(1, groups):
        q = lax.rem(g + k, groups)
        pltpu.make_async_remote_copy(
            src_ref=cbuf.at[q], dst_ref=cbuf.at[q], send_sem=c_send.at[k], recv_sem=c_recv.at[q],
            device_id=(q, d), device_id_type=MESH,
        ).wait_recv()
    for h in range(groups):
        comb_out[:, h * half:(h + 1) * half] = cbuf[h]

    for k in range(1, groups):
        q = lax.rem(g + k, groups)
        lev_copy(k).wait_send()
        for ch in range(chunks):
            x_copy(k, ch).wait_send()
        pltpu.make_async_remote_copy(
            src_ref=cbuf.at[g], dst_ref=cbuf.at[g], send_sem=c_send.at[k], recv_sem=c_recv.at[g],
            device_id=(q, d), device_id_type=MESH,
        ).wait_send()


def owned(levels, count):
    indices = jnp.arange(count, dtype=jnp.int32)
    digits = jnp.stack([indices // 16, indices // 4 % 4, indices % 4])
    return jnp.all(digits[None] <= levels[:, :, None], axis=1).astype(jnp.float32)


def shards(groups, domains, surplus, levels):
    local, subs, cells = surplus.shape
    grids = groups * local
    half = cells // groups
    radices = radices_of(domains)
    sizes = [groups * r if t == 0 else r for t, r in enumerate(radices)]
    dma = pltpu.SemaphoreType.DMA
    chunks = subs // ROWS
    combined, coefficients = pl.pallas_call(
        functools.partial(kernel, groups, radices, local, subs),
        out_shape=(
            jax.ShapeDtypeStruct((subs, cells), F32),
            jax.ShapeDtypeStruct((1, grids), F32),
        ),
        in_specs=[pl.BlockSpec(memory_space=pl.ANY), pl.BlockSpec(memory_space=pltpu.VMEM)],
        out_specs=(pl.BlockSpec(memory_space=pltpu.VMEM), pl.BlockSpec(memory_space=pltpu.VMEM)),
        scratch_shapes=[
            pltpu.VMEM((grids, subs, half), F32),
            pltpu.VMEM((groups, local, 3), jnp.int32),
            pltpu.VMEM((3, grids, 128), jnp.int32),
            pltpu.VMEM((3 * grids, 3 * grids), F32),
            pltpu.VMEM((groups, subs, half), F32),
            dma(()), dma((groups,)), dma((groups,)),
            dma((groups, chunks)), dma((groups, chunks)), dma((groups,)), dma((groups,)),
        ]
        + [pltpu.VMEM((n, grids, 128), F32) for n in sizes]
        + [dma((n,)) for n in sizes]
        + [dma((n,)) for n in sizes],
        compiler_params=pltpu.CompilerParams(collective_id=0, has_side_effects=True),
    )(surplus, levels)
    owners = owned(levels, subs)
    updated = owners[:, :, None] * combined[None]
    return (updated, coefficients.reshape(grids))


def solution(mesh):
    placed = (P("grp", None, "dom"), P("grp", None))
    return jax.shard_map(
        functools.partial(shards, mesh.shape["grp"], mesh.shape["dom"]),
        mesh=mesh, in_specs=placed, out_specs=(P("grp", None, "dom"), P()), check_vma=False,
    )
```

```python
import functools

import jax
import jax.numpy as jnp
from jax import lax
from jax.experimental import pallas as pl
from jax.experimental.pallas import tpu as pltpu
from jax.sharding import PartitionSpec as P

MESH = pl.DeviceIdType.MESH
ROWS = 8
BLOCK = 4
SPREAD = 4
F32 = jnp.float32


def radices_of(size):
    out = []
    while size > 1:
        for r in (4, 2, 3, 5, 7, size):
            if size % r == 0:
                out.append(r)
                size //= r
                break
    return out


def digits_of(sub):
    return (sub // 16).astype(F32), lax.rem(sub // 4, 4).astype(F32), lax.rem(sub, 4).astype(F32)


def split3(x):
    hi = x.astype(jnp.bfloat16)
    rest = x - hi.astype(F32)
    mid = rest.astype(jnp.bfloat16)
    lo = (rest - mid.astype(F32)).astype(jnp.bfloat16)
    return jnp.concatenate([hi, mid, lo], axis=0)


def kernel(groups, radices, local, subs, surplus, levels, comb_out, coef_out, lev_out, *scratch):
    stages = len(radices)
    (xb, lev, lbc, prod, cbuf, local_sem, lev_send, lev_recv, x_send, x_recv, c_send, c_recv) = scratch[:12]
    slots = scratch[12:12 + stages]
    s_send = scratch[12 + stages:12 + 2 * stages]
    s_recv = scratch[12 + 2 * stages:12 + 3 * stages]
    grids = groups * local
    half = xb.shape[-1]
    chunks = subs // ROWS
    g = lax.axis_index("grp")
    d = lax.axis_index("dom")

    members = []
    stride = 1
    for t, r in enumerate(radices):
        digit = lax.rem(d // stride, r)
        base = d - digit * stride
        if t == 0:
            n = groups * r
            mine = g * r + digit
            device = functools.partial(lambda b, r_, q: (q // r_, b + lax.rem(q, r_)), base, r)
        else:
            n = r
            mine = digit
            device = functools.partial(lambda b, st, q: (g, b + q * st), base, stride)
        members.append((n, mine, device))
        stride *= r

    barrier = pltpu.get_barrier_semaphore()
    count = 0
    for n, mine, device in members:
        for k in range(1, n):
            q = lax.rem(mine + k, n)
            pl.semaphore_signal(barrier, inc=1, device_id=device(q), device_id_type=MESH)
            count += 1

    own_cells = pl.ds(pl.multiple_of(g * half, half), half)
    own_copy = pltpu.make_async_copy(
        surplus.at[:, :, own_cells], xb.at[pl.ds(g * local, local)], local_sem
    )
    own_copy.start()
    pl.semaphore_wait(barrier, count)

    def lev_copy(k):
        q = lax.rem(g + k, groups)
        return pltpu.make_async_remote_copy(
            src_ref=levels, dst_ref=lev.at[g], send_sem=lev_send.at[k], recv_sem=lev_recv.at[g],
            device_id=(q, d), device_id_type=MESH,
        )

    def x_copy(k, ch):
        q = lax.rem(g + k, groups)
        rows = pl.ds(pl.multiple_of(ch * ROWS, ROWS), ROWS)
        return pltpu.make_async_remote_copy(
            src_ref=surplus.at[:, rows, pl.ds(pl.multiple_of(q * half, half), half)],
            dst_ref=xb.at[pl.ds(g * local, local), rows],
            send_sem=x_send.at[k, ch], recv_sem=x_recv.at[g, ch],
            device_id=(q, d), device_id_type=MESH,
        )

    def x_arrival(k, ch):
        q = lax.rem(g + k, groups)
        rows = pl.ds(pl.multiple_of(ch * ROWS, ROWS), ROWS)
        block = xb.at[pl.ds(q * local, local), rows]
        return pltpu.make_async_remote_copy(
            src_ref=block, dst_ref=block, send_sem=x_send.at[k, ch], recv_sem=x_recv.at[q, ch],
            device_id=(q, d), device_id_type=MESH,
        )

    for k in range(1, groups):
        lev_copy(k).start()
    for ch in range(chunks):
        for k in range(1, groups):
            x_copy(k, ch).start()

    lev[g] = levels[...]
    for k in range(1, groups):
        q = lax.rem(g + k, groups)
        pltpu.make_async_remote_copy(
            src_ref=lev.at[q], dst_ref=lev.at[q], send_sem=lev_send.at[k], recv_sem=lev_recv.at[q],
            device_id=(q, d), device_id_type=MESH,
        ).wait_recv()
    lev_eye = lax.broadcasted_iota(jnp.int32, (local, local), 0) == lax.broadcasted_iota(
        jnp.int32, (local, local), 1
    )
    for h in range(groups):
        for axis in range(3):
            lev_row = lev[h, axis:axis + 1, :].astype(F32)
            lev_col = jnp.sum(jnp.where(lev_eye, lev_row, 0.0), axis=1, keepdims=True)
            lbc[axis, pl.ds(h * local, local), :] = jnp.broadcast_to(lev_col, (local, 128))
    lev_out[...] = lbc[:, pl.ds(pl.multiple_of(g * local, 8), local), :]
    prod[...] = jnp.zeros_like(prod)
    own_copy.wait()
    flat = xb.reshape(grids * subs, half)

    def gram_chunk(ch, carry):
        for k in range(1, groups):
            x_arrival(k, ch).wait_recv()
        lev0, lev1, lev2 = lbc[0], lbc[1], lbc[2]
        total = jnp.zeros(prod.shape, F32)
        for pair in range(0, ROWS, 2):
            parts = []
            for k in range(pair, pair + 2):
                s = ch * ROWS + k
                x = flat[pl.ds(s, grids, stride=subs), :]
                keep = (
                    (lev0 >= (s // 16).astype(F32))
                    & (lev1 >= lax.rem(s // 4, 4).astype(F32))
                    & (lev2 >= float(k % 4))
                )
                keep = jnp.concatenate([keep] * (half // 128), axis=1) if half > 128 else keep
                parts.append(jnp.where(keep, x, 0.0))
            y = split3(jnp.concatenate(parts, axis=1))
            total += lax.dot_general(y, y, (((1,), (1,)), ((), ())), preferred_element_type=F32)
        prod[...] += total
        return carry

    lax.fori_loop(0, chunks, gram_chunk, 0)

    part = jnp.zeros((grids, grids), F32)
    for a in reversed(range(3)):
        for b in reversed(range(3)):
            part += prod[a * grids:(a + 1) * grids, b * grids:(b + 1) * grids]
    value = jnp.concatenate([part, jnp.zeros((grids, 128 - grids), F32)], axis=1)
    fold = grids // 2
    value = value[:fold] + pltpu.roll(value[fold:], 64, 1)

    for t, (n, mine, device) in enumerate(members):
        buf, send, recv = slots[t], s_send[t], s_recv[t]
        buf[mine] = value
        copies = []
        for k in range(1, n):
            q = lax.rem(mine + k, n)
            copy = pltpu.make_async_remote_copy(
                src_ref=buf.at[mine], dst_ref=buf.at[mine], send_sem=send.at[k], recv_sem=recv.at[mine],
                device_id=device(q), device_id_type=MESH,
            )
            copy.start()
            copies.append(copy)
        for k in range(1, n):
            q = lax.rem(mine + k, n)
            pltpu.make_async_remote_copy(
                src_ref=buf.at[q], dst_ref=buf.at[q], send_sem=send.at[k], recv_sem=recv.at[q],
                device_id=device(q), device_id_type=MESH,
            ).wait_recv()
        value = buf[0]
        for q in range(1, n):
            value = value + buf[q]
        for copy in copies:
            copy.wait_send()

    left = lax.broadcasted_iota(jnp.int32, (fold, 128), 1) < 64
    value = jnp.concatenate(
        [jnp.where(left, value, 0.0), jnp.where(left, pltpu.roll(value, 64, 1), 0.0)], axis=0
    )

    row = lax.broadcasted_iota(jnp.int32, (grids, 128), 0)
    col = lax.broadcasted_iota(jnp.int32, (grids, 128), 1)
    eye = row == col
    diag = jnp.where(eye, value, 0.0)
    diag_col = jnp.sum(diag, axis=1, keepdims=True) + 1e-06
    diag_row = jnp.sum(diag, axis=0, keepdims=True) + 1e-06
    scale_col = 1.0 / jnp.sqrt(diag_col)
    scale_row = 1.0 / jnp.sqrt(diag_row)
    system = scale_col * value * scale_row + jnp.where(eye, 0.1, 0.0)
    system = jnp.where(col == grids, jnp.sqrt(diag_col), jnp.where(col < grids, system, 0.0))
    for first in range(0, grids, BLOCK):
        width = min(BLOCK, grids - first)
        rows = [system[first + j:first + j + 1, :] for j in range(width)]
        cols = [
            jnp.broadcast_to(system[:, first + j:first + j + 1], (grids, 128)) for j in range(width)
        ]
        for j in range(width):
            k = first + j
            inverse = 1.0 / cols[j][k:k + 1, :]
            factor = jnp.where(row == k, 0.0, cols[j] * inverse)
            for m in range(j + 1, width):
                cols[m] = cols[m] - factor * cols[m][k:k + 1, :]
                rows[m] = rows[m] - factor[first + m:first + m + 1, :] * rows[j]
            system = system - factor * rows[j]
    final = jnp.sum(jnp.where(eye, system, 0.0), axis=1, keepdims=True)
    coef = scale_col * (system[:, grids:grids + 1] / final)
    coef_wide = jnp.broadcast_to(coef, (grids, 128))
    coef_out[...] = jnp.sum(jnp.where(eye, coef_wide, 0.0), axis=0, keepdims=True)[:, :grids]

    sub = lax.broadcasted_iota(jnp.int32, (subs, half), 0)
    dig0, dig1, dig2 = digits_of(sub)
    acc = jnp.zeros((subs, half), F32)
    for i in range(grids):
        keep = (
            (lbc[0, i:i + 1, 0:1] >= dig0)
            & (lbc[1, i:i + 1, 0:1] >= dig1)
            & (lbc[2, i:i + 1, 0:1] >= dig2)
        )
        acc += jnp.where(keep, coef_wide[i:i + 1, 0:1], 0.0) * xb[i]
    cbuf[g] = acc
    for k in range(1, groups):
        q = lax.rem(g + k, groups)
        pltpu.make_async_remote_copy(
            src_ref=cbuf.at[g], dst_ref=cbuf.at[g], send_sem=c_send.at[k], recv_sem=c_recv.at[g],
            device_id=(q, d), device_id_type=MESH,
        ).start()
    for k in range(1, groups):
        q = lax.rem(g + k, groups)
        pltpu.make_async_remote_copy(
            src_ref=cbuf.at[q], dst_ref=cbuf.at[q], send_sem=c_send.at[k], recv_sem=c_recv.at[q],
            device_id=(q, d), device_id_type=MESH,
        ).wait_recv()
    for h in range(groups):
        comb_out[:, h * half:(h + 1) * half] = cbuf[h]

    for k in range(1, groups):
        q = lax.rem(g + k, groups)
        lev_copy(k).wait_send()
        for ch in range(chunks):
            x_copy(k, ch).wait_send()
        pltpu.make_async_remote_copy(
            src_ref=cbuf.at[g], dst_ref=cbuf.at[g], send_sem=c_send.at[k], recv_sem=c_recv.at[g],
            device_id=(q, d), device_id_type=MESH,
        ).wait_send()


def spread(combined, coef, lev, updated, coef_out, block, sems):
    local, subs, cells = updated.shape
    coef_out[...] = coef[...]
    dig0, dig1, dig2 = digits_of(lax.broadcasted_iota(jnp.int32, (subs, 128), 0))
    copies = []
    for i in range(local):
        keep = (lev[0, i:i + 1, :] >= dig0) & (lev[1, i:i + 1, :] >= dig1) & (lev[2, i:i + 1, :] >= dig2)
        for c in range(0, cells, 128):
            block[i, :, c:c + 128] = jnp.where(keep, combined[:, c:c + 128], 0.0)
        if (i + 1) % SPREAD == 0 or i + 1 == local:
            n = len(copies)
            part = pl.ds(n * SPREAD, i + 1 - n * SPREAD)
            copy = pltpu.make_async_copy(block.at[part], updated.at[part], sems.at[n])
            copy.start()
            copies.append(copy)
    for copy in copies:
        copy.wait()


def shards(groups, domains, surplus, levels):
    local, subs, cells = surplus.shape
    grids = groups * local
    half = cells // groups
    radices = radices_of(domains)
    sizes = [groups * r if t == 0 else r for t, r in enumerate(radices)]
    dma = pltpu.SemaphoreType.DMA
    chunks = subs // ROWS
    combined, coefficients, lev_wide = pl.pallas_call(
        functools.partial(kernel, groups, radices, local, subs),
        out_shape=(
            jax.ShapeDtypeStruct((subs, cells), F32),
            jax.ShapeDtypeStruct((1, grids), F32),
            jax.ShapeDtypeStruct((3, local, 128), F32),
        ),
        in_specs=[pl.BlockSpec(memory_space=pl.ANY), pl.BlockSpec(memory_space=pltpu.VMEM)],
        out_specs=tuple(pl.BlockSpec(memory_space=pltpu.VMEM) for _ in range(3)),
        scratch_shapes=[
            pltpu.VMEM((grids, subs, half), F32),
            pltpu.VMEM((groups, 3, local), jnp.int32),
            pltpu.VMEM((3, grids, 128), F32),
            pltpu.VMEM((3 * grids, 3 * grids), F32),
            pltpu.VMEM((groups, subs, half), F32),
            dma(()), dma((groups,)), dma((groups,)),
            dma((groups, chunks)), dma((groups, chunks)), dma((groups,)), dma((groups,)),
        ]
        + [pltpu.VMEM((n, grids // 2, 128), F32) for n in sizes]
        + [dma((n,)) for n in sizes]
        + [dma((n,)) for n in sizes],
        compiler_params=pltpu.CompilerParams(collective_id=0, has_side_effects=True),
    )(surplus, levels.T)
    updated, coefficients = pl.pallas_call(
        spread,
        out_shape=(
            jax.ShapeDtypeStruct((local, subs, cells), F32),
            jax.ShapeDtypeStruct((1, grids), F32),
        ),
        in_specs=[pl.BlockSpec(memory_space=pltpu.VMEM)] * 3,
        out_specs=(pl.BlockSpec(memory_space=pl.ANY), pl.BlockSpec(memory_space=pltpu.VMEM)),
        scratch_shapes=[pltpu.VMEM((local, subs, cells), F32), dma((-(-local // SPREAD),))],
    )(combined, coefficients, lev_wide)
    return (updated, coefficients.reshape(grids))


def solution(mesh):
    placed = (P("grp", None, "dom"), P("grp", None))
    return jax.shard_map(
        functools.partial(shards, mesh.shape["grp"], mesh.shape["dom"]),
        mesh=mesh, in_specs=placed, out_specs=(P("grp", None, "dom"), P()), check_vma=False,
    )
```

```python
import functools

import jax
import jax.numpy as jnp
from jax import lax
from jax.experimental import pallas as pl
from jax.experimental.pallas import tpu as pltpu
from jax.sharding import PartitionSpec as P

MESH = pl.DeviceIdType.MESH
ROWS = 8
BLOCK = 8
PIECES = 2
SPREAD = 4
F32 = jnp.float32


def radices_of(size):
    out = []
    while size > 1:
        for r in (4, 2, 3, 5, 7, size):
            if size % r == 0:
                out.append(r)
                size //= r
                break
    return out


def digits_of(sub):
    return (sub // 16).astype(F32), lax.rem(sub // 4, 4).astype(F32), lax.rem(sub, 4).astype(F32)


def partner(mine, k, n):
    if n & (n - 1):
        return lax.rem(mine + k, n)
    other, bit = 0, 1
    while bit < n:
        other = other + lax.rem(lax.rem(mine // bit, 2) + (k // bit) % 2, 2) * bit
        bit *= 2
    return other


def split3(x):
    hi = x.astype(jnp.bfloat16)
    rest = x - hi.astype(F32)
    mid = rest.astype(jnp.bfloat16)
    lo = (rest - mid.astype(F32)).astype(jnp.bfloat16)
    return jnp.concatenate([hi, mid, lo], axis=0)


def kernel(groups, radices, local, subs, surplus, levels, comb_out, coef_out, lev_out, *scratch):
    stages = len(radices)
    (xb, lev, lbc, prod, cbuf, local_sem, lev_send, lev_recv, x_send, x_recv, c_send, c_recv) = scratch[:12]
    slots = scratch[12:12 + stages]
    s_send = scratch[12 + stages:12 + 2 * stages]
    s_recv = scratch[12 + 2 * stages:12 + 3 * stages]
    grids = groups * local
    half = xb.shape[-1]
    chunks = subs // ROWS
    g = lax.axis_index("grp")
    d = lax.axis_index("dom")

    members = []
    stride = 1
    for t, r in enumerate(radices):
        digit = lax.rem(d // stride, r)
        base = d - digit * stride
        if t == 0:
            n = groups * r
            mine = g * r + digit
            device = functools.partial(lambda b, r_, q: (q // r_, b + lax.rem(q, r_)), base, r)
        else:
            n = r
            mine = digit
            device = functools.partial(lambda b, st, q: (g, b + q * st), base, stride)
        members.append((n, mine, device))
        stride *= r

    barrier = pltpu.get_barrier_semaphore()
    count = 0
    for n, mine, device in members:
        for k in range(1, n):
            q = partner(mine, k, n)
            pl.semaphore_signal(barrier, inc=1, device_id=device(q), device_id_type=MESH)
            count += 1

    own_cells = pl.ds(pl.multiple_of(g * half, half), half)
    own_copy = pltpu.make_async_copy(
        surplus.at[:, :, own_cells], xb.at[pl.ds(g * local, local)], local_sem
    )
    own_copy.start()
    pl.semaphore_wait(barrier, count)

    def lev_copy(k):
        q = lax.rem(g + k, groups)
        return pltpu.make_async_remote_copy(
            src_ref=levels, dst_ref=lev.at[g], send_sem=lev_send.at[k], recv_sem=lev_recv.at[g],
            device_id=(q, d), device_id_type=MESH,
        )

    def x_copy(k, ch):
        q = lax.rem(g + k, groups)
        rows = pl.ds(pl.multiple_of(ch * ROWS, ROWS), ROWS)
        return pltpu.make_async_remote_copy(
            src_ref=surplus.at[:, rows, pl.ds(pl.multiple_of(q * half, half), half)],
            dst_ref=xb.at[pl.ds(g * local, local), rows],
            send_sem=x_send.at[k, ch], recv_sem=x_recv.at[g, ch],
            device_id=(q, d), device_id_type=MESH,
        )

    def x_arrival(k, ch):
        q = lax.rem(g + k, groups)
        rows = pl.ds(pl.multiple_of(ch * ROWS, ROWS), ROWS)
        block = xb.at[pl.ds(q * local, local), rows]
        return pltpu.make_async_remote_copy(
            src_ref=block, dst_ref=block, send_sem=x_send.at[k, ch], recv_sem=x_recv.at[q, ch],
            device_id=(q, d), device_id_type=MESH,
        )

    for k in range(1, groups):
        lev_copy(k).start()
    for ch in range(chunks):
        for k in range(1, groups):
            x_copy(k, ch).start()

    lev[g] = levels[...]
    for k in range(1, groups):
        q = lax.rem(g + k, groups)
        pltpu.make_async_remote_copy(
            src_ref=lev.at[q], dst_ref=lev.at[q], send_sem=lev_send.at[k], recv_sem=lev_recv.at[q],
            device_id=(q, d), device_id_type=MESH,
        ).wait_recv()
    lev_eye = lax.broadcasted_iota(jnp.int32, (local, local), 0) == lax.broadcasted_iota(
        jnp.int32, (local, local), 1
    )
    for h in range(groups):
        for axis in range(3):
            lev_row = lev[h, axis:axis + 1, :].astype(F32)
            lev_col = jnp.sum(jnp.where(lev_eye, lev_row, 0.0), axis=1, keepdims=True)
            lbc[axis, pl.ds(h * local, local), :] = jnp.broadcast_to(lev_col, (local, 128))
    lev_out[...] = lbc[:, pl.ds(pl.multiple_of(g * local, 8), local), :]
    prod[...] = jnp.zeros_like(prod)
    own_copy.wait()
    flat = xb.reshape(grids * subs, half)

    def gram_chunk(ch, carry):
        for k in range(1, groups):
            x_arrival(k, ch).wait_recv()
        lev0, lev1, lev2 = lbc[0], lbc[1], lbc[2]
        total = jnp.zeros(prod.shape, F32)
        for pair in range(0, ROWS, 2):
            parts = []
            for k in range(pair, pair + 2):
                s = ch * ROWS + k
                x = flat[pl.ds(s, grids, stride=subs), :]
                keep = (
                    (lev0 >= (s // 16).astype(F32))
                    & (lev1 >= lax.rem(s // 4, 4).astype(F32))
                    & (lev2 >= float(k % 4))
                )
                keep = jnp.concatenate([keep] * (half // 128), axis=1) if half > 128 else keep
                parts.append(jnp.where(keep, x, 0.0))
            y = split3(jnp.concatenate(parts, axis=1))
            total += lax.dot_general(y, y, (((1,), (1,)), ((), ())), preferred_element_type=F32)
        prod[...] += total
        return carry

    lax.fori_loop(0, chunks, gram_chunk, 0)

    part = prod[2 * grids:, :] + prod[grids:2 * grids, :] + prod[:grids, :]
    part = part[:, 2 * grids:] + part[:, grids:2 * grids] + part[:, :grids]
    value = jnp.concatenate([part, jnp.zeros((grids, 128 - grids), F32)], axis=1)
    fold = grids // 2
    value = value[:fold] + pltpu.roll(value[fold:], 64, 1)

    copies = []
    for t, (n, mine, device) in enumerate(members):
        buf, send, recv = slots[t], s_send[t], s_recv[t]
        buf[mine] = value
        for k in reversed(range(1, n)):
            q = partner(mine, k, n)
            copy = pltpu.make_async_remote_copy(
                src_ref=buf.at[mine], dst_ref=buf.at[mine], send_sem=send.at[k], recv_sem=recv.at[mine],
                device_id=device(q), device_id_type=MESH,
            )
            copy.start()
            copies.append(copy)
        for k in range(1, n):
            q = partner(mine, k, n)
            pltpu.make_async_remote_copy(
                src_ref=buf.at[q], dst_ref=buf.at[q], send_sem=send.at[k], recv_sem=recv.at[q],
                device_id=device(q), device_id_type=MESH,
            ).wait_recv()
        value = buf[0]
        for q in range(1, n):
            value = value + buf[q]

    left = lax.broadcasted_iota(jnp.int32, (fold, 128), 1) < 64
    value = jnp.concatenate(
        [jnp.where(left, value, 0.0), jnp.where(left, pltpu.roll(value, 64, 1), 0.0)], axis=0
    )

    row = lax.broadcasted_iota(jnp.int32, (grids, 128), 0)
    col = lax.broadcasted_iota(jnp.int32, (grids, 128), 1)
    eye = row == col
    diag = jnp.where(eye, value, 0.0)
    diag_col = jnp.sum(diag, axis=1, keepdims=True) + 1e-06
    diag_row = jnp.sum(diag, axis=0, keepdims=True) + 1e-06
    scale_col = 1.0 / jnp.sqrt(diag_col)
    scale_row = 1.0 / jnp.sqrt(diag_row)
    system = scale_col * value * scale_row + jnp.where(eye, 0.1, 0.0)
    system = jnp.where(col == grids, jnp.sqrt(diag_col), jnp.where(col < grids, system, 0.0))
    for first in range(0, grids, BLOCK):
        width = min(BLOCK, grids - first)
        rows = [system[first + j:first + j + 1, :] for j in range(width)]
        cols = [
            jnp.broadcast_to(system[:, first + j:first + j + 1], (grids, 128)) for j in range(width)
        ]
        for j in range(width):
            k = first + j
            inverse = 1.0 / cols[j][k:k + 1, :]
            factor = jnp.where(row == k, 0.0, cols[j] * inverse)
            for m in range(j + 1, width):
                cols[m] = cols[m] - factor * cols[m][k:k + 1, :]
                rows[m] = rows[m] - factor[first + m:first + m + 1, :] * rows[j]
            system = system - factor * rows[j]
    final = jnp.sum(jnp.where(eye, system, 0.0), axis=1, keepdims=True)
    coef = scale_col * (system[:, grids:grids + 1] / final)
    coef_wide = jnp.broadcast_to(coef, (grids, 128))
    coef_out[...] = jnp.sum(jnp.where(eye, coef_wide, 0.0), axis=0, keepdims=True)[:, :grids]

    piece = subs // PIECES

    def c_copy(slot, k, p):
        block = cbuf.at[slot, pl.ds(p * piece, piece)]
        return pltpu.make_async_remote_copy(
            src_ref=block, dst_ref=block, send_sem=c_send.at[k, p], recv_sem=c_recv.at[slot, p],
            device_id=(lax.rem(g + k, groups), d), device_id_type=MESH,
        )

    for p in range(PIECES):
        sub = lax.broadcasted_iota(jnp.int32, (piece, half), 0) + p * piece
        dig0, dig1, dig2 = digits_of(sub)
        acc = jnp.zeros((piece, half), F32)
        for i in range(grids):
            keep = (
                (lbc[0, i:i + 1, 0:1] >= dig0)
                & (lbc[1, i:i + 1, 0:1] >= dig1)
                & (lbc[2, i:i + 1, 0:1] >= dig2)
            )
            acc += jnp.where(keep, coef_wide[i:i + 1, 0:1], 0.0) * xb[i, p * piece:(p + 1) * piece]
        cbuf[g, p * piece:(p + 1) * piece] = acc
        for k in range(1, groups):
            c_copy(g, k, p).start()
    for p in range(PIECES):
        for k in range(1, groups):
            c_copy(lax.rem(g + k, groups), k, p).wait_recv()
    for h in range(groups):
        comb_out[:, h * half:(h + 1) * half] = cbuf[h]

    for copy in copies:
        copy.wait_send()
    for k in range(1, groups):
        lev_copy(k).wait_send()
        for ch in range(chunks):
            x_copy(k, ch).wait_send()
        for p in range(PIECES):
            c_copy(g, k, p).wait_send()


def spread(combined, coef, lev, updated, coef_out, block, sems):
    local, subs, cells = updated.shape
    coef_out[...] = coef[...]
    dig0, dig1, dig2 = digits_of(lax.broadcasted_iota(jnp.int32, (subs, 128), 0))
    copies = []
    for i in range(local):
        keep = (lev[0, i:i + 1, :] >= dig0) & (lev[1, i:i + 1, :] >= dig1) & (lev[2, i:i + 1, :] >= dig2)
        for c in range(0, cells, 128):
            block[i, :, c:c + 128] = jnp.where(keep, combined[:, c:c + 128], 0.0)
        if (i + 1) % SPREAD == 0 or i + 1 == local:
            n = len(copies)
            part = pl.ds(n * SPREAD, i + 1 - n * SPREAD)
            copy = pltpu.make_async_copy(block.at[part], updated.at[part], sems.at[n])
            copy.start()
            copies.append(copy)
    for copy in copies:
        copy.wait()


def shards(groups, domains, surplus, levels):
    local, subs, cells = surplus.shape
    grids = groups * local
    half = cells // groups
    radices = radices_of(domains)
    sizes = [groups * r if t == 0 else r for t, r in enumerate(radices)]
    dma = pltpu.SemaphoreType.DMA
    chunks = subs // ROWS
    combined, coefficients, lev_wide = pl.pallas_call(
        functools.partial(kernel, groups, radices, local, subs),
        out_shape=(
            jax.ShapeDtypeStruct((subs, cells), F32),
            jax.ShapeDtypeStruct((1, grids), F32),
            jax.ShapeDtypeStruct((3, local, 128), F32),
        ),
        in_specs=[pl.BlockSpec(memory_space=pl.ANY), pl.BlockSpec(memory_space=pltpu.VMEM)],
        out_specs=tuple(pl.BlockSpec(memory_space=pltpu.VMEM) for _ in range(3)),
        scratch_shapes=[
            pltpu.VMEM((grids, subs, half), F32),
            pltpu.VMEM((groups, 3, local), jnp.int32),
            pltpu.VMEM((3, grids, 128), F32),
            pltpu.VMEM((3 * grids, 3 * grids), F32),
            pltpu.VMEM((groups, subs, half), F32),
            dma(()), dma((groups,)), dma((groups,)),
            dma((groups, chunks)), dma((groups, chunks)), dma((groups, PIECES)), dma((groups, PIECES)),
        ]
        + [pltpu.VMEM((n, grids // 2, 128), F32) for n in sizes]
        + [dma((n,)) for n in sizes]
        + [dma((n,)) for n in sizes],
        compiler_params=pltpu.CompilerParams(collective_id=0, has_side_effects=True),
    )(surplus, levels.T)
    updated, coefficients = pl.pallas_call(
        spread,
        out_shape=(
            jax.ShapeDtypeStruct((local, subs, cells), F32),
            jax.ShapeDtypeStruct((1, grids), F32),
        ),
        in_specs=[pl.BlockSpec(memory_space=pltpu.VMEM)] * 3,
        out_specs=(pl.BlockSpec(memory_space=pl.ANY), pl.BlockSpec(memory_space=pltpu.VMEM)),
        scratch_shapes=[pltpu.VMEM((local, subs, cells), F32), dma((-(-local // SPREAD),))],
    )(combined, coefficients, lev_wide)
    return (updated, coefficients.reshape(grids))


def solution(mesh):
    placed = (P("grp", None, "dom"), P("grp", None))
    return jax.shard_map(
        functools.partial(shards, mesh.shape["grp"], mesh.shape["dom"]),
        mesh=mesh, in_specs=placed, out_specs=(P("grp", None, "dom"), P()), check_vma=False,
    )
```

```python
import functools

import jax
import jax.numpy as jnp
from jax import lax
from jax.experimental import pallas as pl
from jax.experimental.pallas import tpu as pltpu
from jax.sharding import PartitionSpec as P

MESH = pl.DeviceIdType.MESH
ROWS = 8
BLOCK = 16
PIECES = 2
SPREAD = 4
F32 = jnp.float32


def radices_of(size):
    out = []
    while size > 1:
        for r in (4, 2, 3, 5, 7, size):
            if size % r == 0:
                out.append(r)
                size //= r
                break
    return out


def digits_of(sub):
    return (sub // 16).astype(F32), lax.rem(sub // 4, 4).astype(F32), lax.rem(sub, 4).astype(F32)


def split3(x):
    hi = x.astype(jnp.bfloat16)
    rest = x - hi.astype(F32)
    mid = rest.astype(jnp.bfloat16)
    lo = (rest - mid.astype(F32)).astype(jnp.bfloat16)
    return jnp.concatenate([hi, mid, lo], axis=0)


def kernel(groups, radices, local, subs, surplus, levels, comb_out, coef_out, lev_out, *scratch):
    stages = len(radices)
    (xb, lev, lbc, prod, cbuf, local_sem, lev_send, lev_recv, x_send, x_recv, c_send, c_recv) = scratch[:12]
    slots = scratch[12:12 + stages]
    s_send = scratch[12 + stages:12 + 2 * stages]
    s_recv = scratch[12 + 2 * stages:12 + 3 * stages]
    grids = groups * local
    half = xb.shape[-1]
    chunks = subs // ROWS
    g = lax.axis_index("grp")
    d = lax.axis_index("dom")

    members = []
    stride = 1
    for t, r in enumerate(radices):
        digit = lax.rem(d // stride, r)
        base = d - digit * stride
        if t == 0:
            n = groups * r
            mine = g * r + digit
            device = functools.partial(lambda b, r_, q: (q // r_, b + lax.rem(q, r_)), base, r)
        else:
            n = r
            mine = digit
            device = functools.partial(lambda b, st, q: (g, b + q * st), base, stride)
        members.append((n, mine, device))
        stride *= r

    barrier = pltpu.get_barrier_semaphore()
    count = 0
    for n, mine, device in members:
        for k in range(1, n):
            q = lax.rem(mine + k, n)
            pl.semaphore_signal(barrier, inc=1, device_id=device(q), device_id_type=MESH)
            count += 1

    own_cells = pl.ds(pl.multiple_of(g * half, half), half)
    own_copy = pltpu.make_async_copy(
        surplus.at[:, :, own_cells], xb.at[pl.ds(g * local, local)], local_sem
    )
    own_copy.start()
    pl.semaphore_wait(barrier, count)

    def lev_copy(k):
        q = lax.rem(g + k, groups)
        return pltpu.make_async_remote_copy(
            src_ref=levels, dst_ref=lev.at[g], send_sem=lev_send.at[k], recv_sem=lev_recv.at[g],
            device_id=(q, d), device_id_type=MESH,
        )

    def x_copy(k, ch):
        q = lax.rem(g + k, groups)
        rows = pl.ds(pl.multiple_of(ch * ROWS, ROWS), ROWS)
        return pltpu.make_async_remote_copy(
            src_ref=surplus.at[:, rows, pl.ds(pl.multiple_of(q * half, half), half)],
            dst_ref=xb.at[pl.ds(g * local, local), rows],
            send_sem=x_send.at[k, ch], recv_sem=x_recv.at[g, ch],
            device_id=(q, d), device_id_type=MESH,
        )

    def x_arrival(k, ch):
        q = lax.rem(g + k, groups)
        rows = pl.ds(pl.multiple_of(ch * ROWS, ROWS), ROWS)
        block = xb.at[pl.ds(q * local, local), rows]
        return pltpu.make_async_remote_copy(
            src_ref=block, dst_ref=block, send_sem=x_send.at[k, ch], recv_sem=x_recv.at[q, ch],
            device_id=(q, d), device_id_type=MESH,
        )

    for k in range(1, groups):
        lev_copy(k).start()
    for ch in range(chunks):
        for k in range(1, groups):
            x_copy(k, ch).start()

    lev[g] = levels[...]
    for k in range(1, groups):
        q = lax.rem(g + k, groups)
        pltpu.make_async_remote_copy(
            src_ref=lev.at[q], dst_ref=lev.at[q], send_sem=lev_send.at[k], recv_sem=lev_recv.at[q],
            device_id=(q, d), device_id_type=MESH,
        ).wait_recv()
    lev_eye = lax.broadcasted_iota(jnp.int32, (local, local), 0) == lax.broadcasted_iota(
        jnp.int32, (local, local), 1
    )
    for h in range(groups):
        for axis in range(3):
            lev_row = lev[h, axis:axis + 1, :].astype(F32)
            lev_col = jnp.sum(jnp.where(lev_eye, lev_row, 0.0), axis=1, keepdims=True)
            lbc[axis, pl.ds(h * local, local), :] = jnp.broadcast_to(lev_col, (local, 128))
    lev_out[...] = lbc[:, pl.ds(pl.multiple_of(g * local, 8), local), :]
    prod[...] = jnp.zeros_like(prod)
    own_copy.wait()
    flat = xb.reshape(grids * subs, half)

    def gram_chunk(ch, carry):
        for k in range(1, groups):
            x_arrival(k, ch).wait_recv()
        lev0, lev1, lev2 = lbc[0], lbc[1], lbc[2]
        total = jnp.zeros(prod.shape, F32)
        for pair in range(0, ROWS, 2):
            parts = []
            for k in range(pair, pair + 2):
                s = ch * ROWS + k
                x = flat[pl.ds(s, grids, stride=subs), :]
                keep = (
                    (lev0 >= (s // 16).astype(F32))
                    & (lev1 >= lax.rem(s // 4, 4).astype(F32))
                    & (lev2 >= float(k % 4))
                )
                keep = jnp.concatenate([keep] * (half // 128), axis=1) if half > 128 else keep
                parts.append(jnp.where(keep, x, 0.0))
            y = split3(jnp.concatenate(parts, axis=1))
            total += lax.dot_general(y, y, (((1,), (1,)), ((), ())), preferred_element_type=F32)
        prod[...] += total
        return carry

    lax.fori_loop(0, chunks, gram_chunk, 0)

    part = prod[2 * grids:, :] + prod[grids:2 * grids, :] + prod[:grids, :]
    part = part[:, 2 * grids:] + part[:, grids:2 * grids] + part[:, :grids]
    value = jnp.concatenate([part, jnp.zeros((grids, 128 - grids), F32)], axis=1)
    fold = grids // 2
    value = value[:fold] + pltpu.roll(value[fold:], 64, 1)

    copies = []
    for t, (n, mine, device) in enumerate(members):
        buf, send, recv = slots[t], s_send[t], s_recv[t]
        buf[mine] = value
        for k in range(1, n):
            q = lax.rem(mine + k, n)
            copy = pltpu.make_async_remote_copy(
                src_ref=buf.at[mine], dst_ref=buf.at[mine], send_sem=send.at[k], recv_sem=recv.at[mine],
                device_id=device(q), device_id_type=MESH,
            )
            copy.start()
            copies.append(copy)
        for k in range(1, n):
            q = lax.rem(mine + k, n)
            pltpu.make_async_remote_copy(
                src_ref=buf.at[q], dst_ref=buf.at[q], send_sem=send.at[k], recv_sem=recv.at[q],
                device_id=device(q), device_id_type=MESH,
            ).wait_recv()
        value = buf[0]
        for q in range(1, n):
            value = value + buf[q]

    left = lax.broadcasted_iota(jnp.int32, (fold, 128), 1) < 64
    value = jnp.concatenate(
        [jnp.where(left, value, 0.0), jnp.where(left, pltpu.roll(value, 64, 1), 0.0)], axis=0
    )

    row = lax.broadcasted_iota(jnp.int32, (grids, 128), 0)
    col = lax.broadcasted_iota(jnp.int32, (grids, 128), 1)
    eye = row == col
    diag = jnp.where(eye, value, 0.0)
    diag_col = jnp.sum(diag, axis=1, keepdims=True) + 1e-06
    diag_row = jnp.sum(diag, axis=0, keepdims=True) + 1e-06
    scale_col = 1.0 / jnp.sqrt(diag_col)
    scale_row = 1.0 / jnp.sqrt(diag_row)
    system = scale_col * value * scale_row + jnp.where(eye, 0.1, 0.0)
    system = jnp.where(col == grids, jnp.sqrt(diag_col), jnp.where(col < grids, system, 0.0))
    for first in range(0, grids, BLOCK):
        width = min(BLOCK, grids - first)
        rows = [system[first + j:first + j + 1, :] for j in range(width)]
        cols = [
            jnp.broadcast_to(system[:, first + j:first + j + 1], (grids, 128)) for j in range(width)
        ]
        for j in range(width):
            k = first + j
            inverse = 1.0 / cols[j][k:k + 1, :]
            factor = jnp.where(row == k, 0.0, cols[j] * inverse)
            for m in range(j + 1, width):
                cols[m] = cols[m] - factor * cols[m][k:k + 1, :]
                rows[m] = rows[m] - factor[first + m:first + m + 1, :] * rows[j]
            system = system - factor * rows[j]
    final = jnp.sum(jnp.where(eye, system, 0.0), axis=1, keepdims=True)
    coef = scale_col * (system[:, grids:grids + 1] / final)
    coef_wide = jnp.broadcast_to(coef, (grids, 128))
    coef_out[...] = jnp.sum(jnp.where(eye, coef_wide, 0.0), axis=0, keepdims=True)[:, :grids]

    piece = subs // PIECES

    def c_copy(slot, k, p):
        block = cbuf.at[slot, pl.ds(p * piece, piece)]
        return pltpu.make_async_remote_copy(
            src_ref=block, dst_ref=block, send_sem=c_send.at[k, p], recv_sem=c_recv.at[slot, p],
            device_id=(lax.rem(g + k, groups), d), device_id_type=MESH,
        )

    for p in range(PIECES):
        sub = lax.broadcasted_iota(jnp.int32, (piece, half), 0) + p * piece
        dig0, dig1, dig2 = digits_of(sub)
        acc = jnp.zeros((piece, half), F32)
        for i in range(grids):
            keep = (
                (lbc[0, i:i + 1, 0:1] >= dig0)
                & (lbc[1, i:i + 1, 0:1] >= dig1)
                & (lbc[2, i:i + 1, 0:1] >= dig2)
            )
            acc += jnp.where(keep, coef_wide[i:i + 1, 0:1], 0.0) * xb[i, p * piece:(p + 1) * piece]
        cbuf[g, p * piece:(p + 1) * piece] = acc
        for k in range(1, groups):
            c_copy(g, k, p).start()
    for p in range(PIECES):
        for k in range(1, groups):
            c_copy(lax.rem(g + k, groups), k, p).wait_recv()
    for h in range(groups):
        comb_out[:, h * half:(h + 1) * half] = cbuf[h]

    for copy in copies:
        copy.wait_send()
    for k in range(1, groups):
        lev_copy(k).wait_send()
        for ch in range(chunks):
            x_copy(k, ch).wait_send()
        for p in range(PIECES):
            c_copy(g, k, p).wait_send()


def spread(combined, coef, lev, updated, coef_out, block, sems):
    local, subs, cells = updated.shape
    coef_out[...] = coef[...]
    dig0, dig1, dig2 = digits_of(lax.broadcasted_iota(jnp.int32, (subs, 128), 0))
    copies = []
    for i in range(local):
        keep = (lev[0, i:i + 1, :] >= dig0) & (lev[1, i:i + 1, :] >= dig1) & (lev[2, i:i + 1, :] >= dig2)
        for c in range(0, cells, 128):
            block[i, :, c:c + 128] = jnp.where(keep, combined[:, c:c + 128], 0.0)
        if (i + 1) % SPREAD == 0 or i + 1 == local:
            n = len(copies)
            part = pl.ds(n * SPREAD, i + 1 - n * SPREAD)
            copy = pltpu.make_async_copy(block.at[part], updated.at[part], sems.at[n])
            copy.start()
            copies.append(copy)
    for copy in copies:
        copy.wait()


def shards(groups, domains, surplus, levels):
    local, subs, cells = surplus.shape
    grids = groups * local
    half = cells // groups
    radices = radices_of(domains)
    sizes = [groups * r if t == 0 else r for t, r in enumerate(radices)]
    dma = pltpu.SemaphoreType.DMA
    chunks = subs // ROWS
    combined, coefficients, lev_wide = pl.pallas_call(
        functools.partial(kernel, groups, radices, local, subs),
        out_shape=(
            jax.ShapeDtypeStruct((subs, cells), F32),
            jax.ShapeDtypeStruct((1, grids), F32),
            jax.ShapeDtypeStruct((3, local, 128), F32),
        ),
        in_specs=[pl.BlockSpec(memory_space=pl.ANY), pl.BlockSpec(memory_space=pltpu.VMEM)],
        out_specs=tuple(pl.BlockSpec(memory_space=pltpu.VMEM) for _ in range(3)),
        scratch_shapes=[
            pltpu.VMEM((grids, subs, half), F32),
            pltpu.VMEM((groups, 3, local), jnp.int32),
            pltpu.VMEM((3, grids, 128), F32),
            pltpu.VMEM((3 * grids, 3 * grids), F32),
            pltpu.VMEM((groups, subs, half), F32),
            dma(()), dma((groups,)), dma((groups,)),
            dma((groups, chunks)), dma((groups, chunks)), dma((groups, PIECES)), dma((groups, PIECES)),
        ]
        + [pltpu.VMEM((n, grids // 2, 128), F32) for n in sizes]
        + [dma((n,)) for n in sizes]
        + [dma((n,)) for n in sizes],
        compiler_params=pltpu.CompilerParams(collective_id=0, has_side_effects=True),
    )(surplus, levels.T)
    updated, coefficients = pl.pallas_call(
        spread,
        out_shape=(
            jax.ShapeDtypeStruct((local, subs, cells), F32),
            jax.ShapeDtypeStruct((1, grids), F32),
        ),
        in_specs=[pl.BlockSpec(memory_space=pltpu.VMEM)] * 3,
        out_specs=(pl.BlockSpec(memory_space=pl.ANY), pl.BlockSpec(memory_space=pltpu.VMEM)),
        scratch_shapes=[pltpu.VMEM((local, subs, cells), F32), dma((-(-local // SPREAD),))],
    )(combined, coefficients, lev_wide)
    return (updated, coefficients.reshape(grids))


def solution(mesh):
    placed = (P("grp", None, "dom"), P("grp", None))
    return jax.shard_map(
        functools.partial(shards, mesh.shape["grp"], mesh.shape["dom"]),
        mesh=mesh, in_specs=placed, out_specs=(P("grp", None, "dom"), P()), check_vma=False,
    )
```
